32 devices in a mesh: seq: 8 (over z, y), layer: 4 (over x, core).
Axes of the slice: x: 2, y: 2, z: 4, core: 2. Of those that a mesh axis runs over, the one named last changes fastest.
Arguments:
- gradients: bfloat16 [2048, 4096], P('seq', 'layer'), may hold values from -6 to 6
- projection: bfloat16 [4096, 8192], P('layer', 'seq'), may hold values from -0.09375 to 0.09375
- queries: bfloat16 [256, 8192], P(None, 'seq'), may hold values from -6 to 6
Outputs:
- scores: float32 [2048, 256], P(('seq', 'layer'))
The draws below stay inside these ranges and needn't reach their ends.
All inputs are finite; a program needn't handle non-finite values.
Results may differ from the reference program's by a relative error of at most 0.0029.
Values may be sent and summed in bfloat16 or wider, within the bound.
A program may use at most 128 MiB of HBM per device.

```python
import math
import jax
import jax.numpy as jnp
from jax import lax

FEAT = 4096
K = 8192
Q = 256
S = 2048


def level_of(own_key, extent, split, low, high):
    gain = 1.0
    for position, blocks in split:
        steps = jax.random.uniform(jax.random.fold_in(jax.random.fold_in(own_key, 6), position), (blocks,), jnp.float32, low / len(split), high / len(split))
        gain = gain * jnp.repeat(jnp.exp(steps), extent[position] // blocks).reshape((-1,) + (1,) * (len(extent) - 1 - position))
    return gain


def centred(key, extent, spread, bound, shards=(), held_as=jnp.bfloat16):
    factor_of = level_of(key, extent, shards, -0.22, 0.18) if shards else 1.0
    array = jax.random.normal(key, extent, jnp.float32) * spread * factor_of
    return jnp.minimum(jnp.maximum(array, -bound), bound).astype(held_as)


def setup_inputs(seed: int = 0) -> dict:
    keys = jax.random.split(jax.random.key(seed), 4)
    gradients = centred(keys[0], (S, FEAT), 1.0, 6.0, ((0, 8), (1, 4)))
    projection = centred(keys[1], (FEAT, K), FEAT ** -0.5, 0.09375, ((0, 4), (1, 8)))
    queries = centred(keys[2], (Q, K), 1.0, 6.0, ((1, 8),))
    return dict(gradients=gradients, projection=projection, queries=queries)


epsilon = 1e-06

def reference(gradients, projection, queries):
    sketch = jnp.dot(gradients, projection, preferred_element_type=jnp.float32).astype(jnp.bfloat16)
    sketch_wide = sketch.astype(jnp.float32)
    row_squares = lax.optimization_barrier(jnp.sum(sketch_wide * sketch_wide, axis=1))
    query_wide = queries.astype(jnp.float32)
    query_squares = lax.optimization_barrier(jnp.sum(query_wide * query_wide, axis=1))
    products = lax.dot_general(sketch, queries, (((1,), (1,)), ((), ())), preferred_element_type=jnp.float32)
    return math.sqrt(K) * products * lax.rsqrt(row_squares + epsilon)[:, None] * lax.rsqrt(query_squares + epsilon)[None, :]
```

```python
import functools
import math

import jax
import jax.numpy as jnp
from jax import lax
from jax.experimental import pallas as pl
from jax.experimental.pallas import tpu as pltpu
from jax.sharding import PartitionSpec as P

epsilon = 1e-06
VMEM_BYTES = 60 * 2**20
MESH = pl.DeviceIdType.MESH


def scaled(width, products, row_squares, query_squares):
    return (
        math.sqrt(width)
        * products
        * lax.rsqrt(row_squares + epsilon)
        * lax.rsqrt(query_squares + epsilon)
    )


def kernel(
    groups, layers,
    g_ref, p_ref, q_ref, out_ref,
    gbuf, pother, qt, totals, xsend, xrecv, sbuf, rbuf,
    local_sem, core_sem, pair_sem, gsend, grecv, xsend_sem, xrecv_sem, rsend_sem, rrecv_sem,
):
    inner = 2
    outer = groups // inner
    banks = layers // 2
    rows = g_ref.shape[2]
    columns = p_ref.shape[1]
    asked = q_ref.shape[0]
    me, layer = lax.axis_index("seq"), lax.axis_index("layer")
    z, y = me // inner, me % inner
    x, c = layer // 2, layer % 2
    partner = x * 2 + 1 - c

    barrier = pltpu.get_barrier_semaphore()
    for step in range(1, groups):
        pl.semaphore_signal(
            barrier, inc=1, device_id=((me + step) % groups, layer), device_id_type=MESH
        )
    for step in range(1, layers):
        pl.semaphore_signal(
            barrier, inc=1, device_id=(me, (layer + step) % layers), device_id_type=MESH
        )
    pl.semaphore_wait(barrier, groups + layers - 2)

    def remote(src, dst, send, recv, group, layer_to):
        return pltpu.make_async_remote_copy(
            src_ref=src, dst_ref=dst, send_sem=send, recv_sem=recv,
            device_id=(group, layer_to), device_id_type=MESH,
        )

    own = pltpu.make_async_copy(g_ref.at[:, c], gbuf.at[me, 0], local_sem)
    own.start()
    swap_g = remote(
        g_ref.at[:, 1 - c], gbuf.at[me, 1], core_sem, grecv.at[me, 1], me, partner
    )
    swap_g.start()
    swap_p = remote(p_ref, pother, pair_sem.at[0], pair_sem.at[1], me, partner)
    swap_p.start()
    own.wait()

    reach = jnp.minimum(z, outer - 1 - z)

    def source(t):
        half = (t + 1) // 2
        near = z + half * (2 * (t % 2) - 1)
        far = jnp.where(z <= outer - 1 - z, t, outer - 1 - t)
        return jnp.where(t <= 2 * reach, near, far)

    def chunk(block, part, link, group):
        return remote(
            gbuf.at[block, part], gbuf.at[block, part],
            gsend.at[block, part, link], grecv.at[block, part], group, layer,
        )

    def links(src, act):
        block = src * inner + y

        def send(part):
            act(chunk(block, part, 0, z * inner + 1 - y))

            @pl.when((src <= z) & (z < outer - 1))
            def _():
                act(chunk(block, part, 1, (z + 1) * inner + y))

            @pl.when((src >= z) & (z > 0))
            def _():
                act(chunk(block, part, 2, (z - 1) * inner + y))

        return send

    tile = min(columns, 256)

    def multiply(block):
        @pl.loop(0, columns // tile)
        def _(k):
            cols = pl.ds(pl.multiple_of(k * tile, tile), tile)
            first = gbuf[block, 0].reshape(banks * rows, -1)
            second = gbuf[block, 1].reshape(banks * rows, -1)
            total = jnp.dot(first, p_ref[:, cols], preferred_element_type=jnp.float32)
            total += jnp.dot(second, pother[:, cols], preferred_element_type=jnp.float32)
            total = total.reshape(banks, rows, tile)
            totals[block, :, :, cols] = total
            xsend[block, :, :, cols] = total.astype(jnp.bfloat16)

        for step in range(1, banks):
            exchange(block, step).start()

    def exchange(block, step):
        to = (x + step) % banks
        return remote(
            xsend.at[block, to], xrecv.at[block, step - 1],
            xsend_sem.at[block, step - 1], xrecv_sem.at[block, step - 1],
            me, to * 2 + c,
        )

    def deliver(block):
        return remote(
            sbuf.at[block], rbuf.at[me], rsend_sem.at[block], rrecv_sem.at[me], block, layer
        )

    def finish(block):
        sketch = totals[block, x]
        for step in range(1, banks):
            exchange(block, step).wait_recv()
            sketch += xrecv[block, step - 1].astype(jnp.float32)
        high = sketch.astype(jnp.bfloat16)
        low = (sketch - high.astype(jnp.float32)).astype(jnp.bfloat16)
        both = jnp.dot(
            jnp.concatenate([high, low], axis=0), qt[...], preferred_element_type=jnp.float32
        )
        squares = jnp.sum(sketch * sketch, axis=1, keepdims=True)
        sbuf[block, :rows] = both[:rows] + both[rows:]
        sbuf[block, rows : rows + 8, :rows] = jnp.broadcast_to(squares, (rows, 128)).T[:8]

        @pl.when(block != me)
        def _():
            deliver(block).start()

    wide = q_ref[...].T
    qt[...] = wide
    wide = wide.astype(jnp.float32)
    query_part = jnp.sum(wide * wide, axis=0, keepdims=True)

    @pl.loop(0, groups)
    def _(block):
        sbuf[block, rows + 8 :] = jnp.broadcast_to(query_part, (8, asked))

    @pl.loop(0, outer + 2)
    def _(t):
        @pl.when(t < outer)
        def _():
            src = source(t)
            block = src * inner + y
            for part in range(2):
                if part == 0:
                    @pl.when(t > 0)
                    def _():
                        chunk(block, 0, 0, me).wait_recv()
                else:
                    chunk(block, 1, 0, me).wait_recv()
                links(src, lambda copy: copy.start())(part)

            @pl.when(t == 0)
            def _():
                swap_p.wait_recv()

            multiply(block)

        @pl.when((t >= 1) & (t <= outer))
        def _():
            finish(source(t - 1) * inner + y)
            block = source(t - 1) * inner + 1 - y
            for part in range(2):
                chunk(block, part, 0, me).wait_recv()
            multiply(block)

        @pl.when(t >= 2)
        def _():
            finish(source(t - 2) * inner + 1 - y)

    products = sbuf[me]

    def collect(step, total):
        block = (me + step) % groups
        remote(
            sbuf.at[block], rbuf.at[block], rsend_sem.at[block], rrecv_sem.at[block],
            block, layer,
        ).wait_recv()
        return total + rbuf[block]

    products = lax.fori_loop(1, groups, collect, products)
    squares = jnp.broadcast_to(products[rows : rows + 1, :rows], (128, rows)).T[:, :1]
    out_ref[...] = scaled(
        columns * groups, products[:rows], squares, products[rows + 8 : rows + 9]
    )

    swap_g.wait_send()
    swap_p.wait_send()

    @pl.loop(0, outer)
    def _(t):
        src = source(t)
        for part in range(2):
            links(src, lambda copy: copy.wait_send())(part)

    @pl.loop(0, groups)
    def _(block):
        for step in range(1, banks):
            exchange(block, step).wait_send()

        @pl.when(block != me)
        def _():
            deliver(block).wait_send()


def scratch(groups, layers, gradients, projection, queries):
    banks, rows = layers // 2, gradients[0] // layers
    features, columns = projection
    asked = queries[0]
    message = (groups, rows + 16, asked)
    return [
        ((groups, 2, banks, rows, features), jnp.bfloat16),
        ((features, columns), jnp.bfloat16),
        ((columns, asked), jnp.bfloat16),
        ((groups, banks, rows, columns), jnp.float32),
        ((groups, banks, rows, columns), jnp.bfloat16),
        ((groups, max(banks - 1, 1), rows, columns), jnp.bfloat16),
        (message, jnp.float32),
        (message, jnp.float32),
    ]


def fused(groups, layers, gradients, projection, queries):
    banks = layers // 2
    rows = gradients.shape[0] // layers
    buffers = scratch(groups, layers, gradients.shape, projection.shape, queries.shape)
    dma = pltpu.SemaphoreType.DMA
    spread = max(banks - 1, 1)
    return pl.pallas_call(
        functools.partial(kernel, groups, layers),
        out_shape=jax.ShapeDtypeStruct((rows, queries.shape[0]), jnp.float32),
        in_specs=[pl.BlockSpec(memory_space=pltpu.VMEM)] * 3,
        out_specs=pl.BlockSpec(memory_space=pltpu.VMEM),
        scratch_shapes=[pltpu.VMEM(shape, kind) for shape, kind in buffers]
        + [
            dma, dma, dma((2,)), dma((groups, 2, 3)), dma((groups, 2)),
            dma((groups, spread)), dma((groups, spread)), dma((groups,)), dma((groups,)),
        ],
        compiler_params=pltpu.CompilerParams(
            collective_id=0, has_side_effects=True, vmem_limit_bytes=VMEM_BYTES
        ),
    )(gradients.reshape(banks, 2, rows, gradients.shape[1]), projection, queries)


def plain(groups, layers, gradients, projection, queries):
    quarter = gradients.shape[0] // layers
    partial_value = jnp.dot(
        lax.all_gather(gradients, "seq", axis=0, tiled=True),
        projection,
        preferred_element_type=jnp.float32,
    )
    partial_value = partial_value.reshape(groups, layers, quarter, projection.shape[1])
    summed = lax.psum_scatter(partial_value, "layer", scatter_dimension=1, tiled=True)
    sketch = summed.reshape(groups * quarter, projection.shape[1]).astype(jnp.bfloat16)
    sketch_wide = sketch.astype(jnp.float32)
    row_squares = lax.psum_scatter(
        jnp.sum(sketch_wide * sketch_wide, axis=1), "seq", scatter_dimension=0, tiled=True
    )
    query_wide = queries.astype(jnp.float32)
    query_squares = lax.psum(jnp.sum(query_wide * query_wide, axis=1), "seq")
    products = lax.psum_scatter(
        lax.dot_general(
            sketch, queries, (((1,), (1,)), ((), ())), preferred_element_type=jnp.float32
        ),
        "seq",
        scatter_dimension=0,
        tiled=True,
    )
    width = projection.shape[1] * groups
    return scaled(width, products, row_squares[:, None], query_squares[None, :])


def shards(gradients, projection, queries):
    layers = lax.axis_size("layer")
    groups = lax.axis_size("seq")
    rows = gradients.shape[0] // layers
    needed = sum(
        math.prod(shape) * jnp.dtype(kind).itemsize
        for shape, kind in scratch(
            groups, layers, gradients.shape, projection.shape, queries.shape
        )
    ) + 2 * (gradients.size + projection.size + queries.size)
    fits = (
        groups % 2 == 0
        and layers % 2 == 0
        and rows % 16 == 0
        and rows <= min(128, queries.shape[0])
        and needed < VMEM_BYTES - 8 * 2**20
    )
    path = fused if fits else plain
    return path(groups, layers, gradients, projection, queries)


def solution(mesh):
    placed = (P("seq", "layer"), P("layer", "seq"), P(None, "seq"))
    return jax.shard_map(
        shards, mesh=mesh, in_specs=placed, out_specs=P(("seq", "layer"), None), check_vma=False
    )
```

```python
import functools
import math

import jax
import jax.numpy as jnp
from jax import lax
from jax.experimental import pallas as pl
from jax.experimental.pallas import tpu as pltpu
from jax.sharding import PartitionSpec as P

epsilon = 1e-06
VMEM_BYTES = 60 * 2**20
MESH = pl.DeviceIdType.MESH


def scaled(width, products, row_squares, query_squares):
    return (
        math.sqrt(width)
        * products
        * lax.rsqrt(row_squares + epsilon)
        * lax.rsqrt(query_squares + epsilon)
    )


def kernel(
    groups, layers,
    g_hbm, p_hbm, q_hbm, out_ref,
    p_ref, q_ref, gbuf, pother, qt, totals, xsend, xrecv, sbuf, rbuf,
    local_sem, core_sem, pair_sem, gsend, grecv, xsend_sem, xrecv_sem, rsend_sem, rrecv_sem,
):
    inner = 2
    outer = groups // inner
    banks = layers // 2
    rows = g_hbm.shape[2]
    columns = p_ref.shape[1]
    asked = q_ref.shape[0]
    me, layer = lax.axis_index("seq"), lax.axis_index("layer")
    z, y = me // inner, me % inner
    x, c = layer // 2, layer % 2
    partner = x * 2 + 1 - c

    own = pltpu.make_async_copy(g_hbm.at[:, c], gbuf.at[me, 0], local_sem.at[0])
    own.start()
    load_p = pltpu.make_async_copy(p_hbm, p_ref, local_sem.at[1])
    load_p.start()
    load_q = pltpu.make_async_copy(q_hbm, q_ref, local_sem.at[2])
    load_q.start()

    barrier = pltpu.get_barrier_semaphore()

    def greet(group, layer_to):
        pl.semaphore_signal(
            barrier, inc=1, device_id=(group, layer_to), device_id_type=MESH
        )

    greet(me, partner)
    greet(z * inner + 1 - y, layer)
    for step in range(1, banks):
        greet(me, (x + step) % banks * 2 + c)

    @pl.when(z > 0)
    def _():
        greet(me - inner, layer)

    @pl.when(z < outer - 1)
    def _():
        greet(me + inner, layer)

    ends = jnp.minimum(z, 1) + jnp.minimum(outer - 1 - z, 1)
    pl.semaphore_wait(barrier, banks + 1 + ends)

    def remote(src, dst, send, recv, group, layer_to):
        return pltpu.make_async_remote_copy(
            src_ref=src, dst_ref=dst, send_sem=send, recv_sem=recv,
            device_id=(group, layer_to), device_id_type=MESH,
        )

    swap_g = remote(
        g_hbm.at[:, 1 - c], gbuf.at[me, 1], core_sem, grecv.at[me, 1], me, partner
    )
    swap_g.start()

    reach = jnp.minimum(z, outer - 1 - z)

    def source(t):
        half = (t + 1) // 2
        near = z + half * (2 * (t % 2) - 1)
        far = jnp.where(z <= outer - 1 - z, t, outer - 1 - t)
        return jnp.where(t <= 2 * reach, near, far)

    def chunk(block, part, link, group):
        return remote(
            gbuf.at[block, part], gbuf.at[block, part],
            gsend.at[block, part, link], grecv.at[block, part], group, layer,
        )

    up, down = z < outer - 1, z > 0

    def relay(src, part, act):
        block = src * inner + y

        @pl.when((part == 0) | (src == z) | ((src > 0) & (src < outer - 1)))
        def _():
            act(chunk(block, part, 0, z * inner + 1 - y))

        @pl.when((src <= z) & up)
        def _():
            act(chunk(block, part, 1, me + inner))

        @pl.when((src >= z) & down)
        def _():
            act(chunk(block, part, 2, me - inner))

    def relay_other(src, act):
        block = src * inner + 1 - y

        @pl.when((src == 0) & up)
        def _():
            act(chunk(block, 1, 1, me + inner))

        @pl.when((src == outer - 1) & down)
        def _():
            act(chunk(block, 1, 2, me - inner))

    def start(copy):
        copy.start()

    def drain(copy):
        copy.wait_send()

    tile = min(columns, 256)

    def multiply(block):
        @pl.loop(0, columns // tile)
        def _(k):
            cols = pl.ds(pl.multiple_of(k * tile, tile), tile)
            first = gbuf[block, 0].reshape(banks * rows, -1)
            second = gbuf[block, 1].reshape(banks * rows, -1)
            total = jnp.dot(first, p_ref[:, cols], preferred_element_type=jnp.float32)
            total += jnp.dot(second, pother[:, cols], preferred_element_type=jnp.float32)
            total = total.reshape(banks, rows, tile)
            totals[block, :, :, cols] = total
            xsend[block, :, :, cols] = total.astype(jnp.bfloat16)

        for step in range(1, banks):
            exchange(block, step).start()

    def exchange(block, step):
        to = (x + step) % banks
        return remote(
            xsend.at[block, to], xrecv.at[block, step - 1],
            xsend_sem.at[block, step - 1], xrecv_sem.at[block, step - 1],
            me, to * 2 + c,
        )

    def deliver(block):
        return remote(
            sbuf.at[block], rbuf.at[me], rsend_sem.at[block], rrecv_sem.at[me], block, layer
        )

    def finish(block):
        sketch = totals[block, x]
        for step in range(1, banks):
            exchange(block, step).wait_recv()
            sketch += xrecv[block, step - 1].astype(jnp.float32)
        high = sketch.astype(jnp.bfloat16)
        low = (sketch - high.astype(jnp.float32)).astype(jnp.bfloat16)
        both = jnp.dot(
            jnp.concatenate([high, low], axis=0), qt[...], preferred_element_type=jnp.float32
        )
        squares = jnp.sum(sketch * sketch, axis=1, keepdims=True)
        sbuf[block, :rows] = both[:rows] + both[rows:]
        sbuf[block, rows : rows + 1, :rows] = jnp.broadcast_to(squares, (rows, 128)).T[:1]

        @pl.when(block != me)
        def _():
            deliver(block).start()

    own.wait()
    relay(z, 0, start)
    swap_p = remote(p_hbm, pother, pair_sem.at[0], pair_sem.at[1], me, partner)
    swap_p.start()
    chunk(me, 1, 0, me).wait_recv()
    relay(z, 1, start)
    load_q.wait()

    wide = q_ref[...].T
    qt[...] = wide
    wide = wide.astype(jnp.float32)
    query_part = jnp.sum(wide * wide, axis=0, keepdims=True)

    @pl.loop(0, groups)
    def _(block):
        sbuf[block, rows + 1 : rows + 2] = query_part

    load_p.wait()
    swap_p.wait_recv()

    @pl.loop(0, outer + 2)
    def _(t):
        @pl.when(t < outer)
        def _():
            src = source(t)
            block = src * inner + y
            @pl.when(t > 0)
            def _():
                for part in range(2):
                    chunk(block, part, 0, me).wait_recv()
                    relay(src, part, start)

            multiply(block)

        @pl.when((t >= 1) & (t <= outer))
        def _():
            finish(source(t - 1) * inner + y)
            block = source(t - 1) * inner + 1 - y
            for part in range(2):
                chunk(block, part, 0, me).wait_recv()
            relay_other(source(t - 1), start)
            multiply(block)

        @pl.when(t >= 2)
        def _():
            finish(source(t - 2) * inner + 1 - y)

    products = sbuf[me]

    def collect(step, total):
        block = (me + step) % groups
        remote(
            sbuf.at[block], rbuf.at[block], rsend_sem.at[block], rrecv_sem.at[block],
            block, layer,
        ).wait_recv()
        return total + rbuf[block]

    products = lax.fori_loop(1, groups, collect, products)
    squares = jnp.broadcast_to(products[rows : rows + 1, :rows], (128, rows)).T[:, :1]
    out_ref[...] = scaled(
        columns * groups, products[:rows], squares, products[rows + 1 : rows + 2]
    )

    swap_g.wait_send()
    swap_p.wait_send()

    @pl.loop(0, outer)
    def _(t):
        src = source(t)
        for part in range(2):
            relay(src, part, drain)
        relay_other(src, drain)

    @pl.loop(0, groups)
    def _(block):
        for step in range(1, banks):
            exchange(block, step).wait_send()

        @pl.when(block != me)
        def _():
            deliver(block).wait_send()


def scratch(groups, layers, gradients, projection, queries):
    banks, rows = layers // 2, gradients[0] // layers
    features, columns = projection
    asked = queries[0]
    message = (groups, rows + 8, asked)
    return [
        ((features, columns), jnp.bfloat16),
        ((asked, columns), jnp.bfloat16),
        ((groups, 2, banks, rows, features), jnp.bfloat16),
        ((features, columns), jnp.bfloat16),
        ((columns, asked), jnp.bfloat16),
        ((groups, banks, rows, columns), jnp.float32),
        ((groups, banks, rows, columns), jnp.bfloat16),
        ((groups, max(banks - 1, 1), rows, columns), jnp.bfloat16),
        (message, jnp.float32),
        (message, jnp.float32),
    ]


def fused(groups, layers, gradients, projection, queries):
    banks = layers // 2
    rows = gradients.shape[0] // layers
    buffers = scratch(groups, layers, gradients.shape, projection.shape, queries.shape)
    dma = pltpu.SemaphoreType.DMA
    spread = max(banks - 1, 1)
    return pl.pallas_call(
        functools.partial(kernel, groups, layers),
        out_shape=jax.ShapeDtypeStruct((rows, queries.shape[0]), jnp.float32),
        in_specs=[pl.BlockSpec(memory_space=pl.ANY)] * 3,
        out_specs=pl.BlockSpec(memory_space=pltpu.VMEM),
        scratch_shapes=[pltpu.VMEM(shape, kind) for shape, kind in buffers]
        + [
            dma((3,)), dma, dma((2,)), dma((groups, 2, 3)), dma((groups, 2)),
            dma((groups, spread)), dma((groups, spread)), dma((groups,)), dma((groups,)),
        ],
        compiler_params=pltpu.CompilerParams(
            collective_id=0, has_side_effects=True, vmem_limit_bytes=VMEM_BYTES
        ),
    )(gradients.reshape(banks, 2, rows, gradients.shape[1]), projection, queries)


def plain(groups, layers, gradients, projection, queries):
    quarter = gradients.shape[0] // layers
    partial_value = jnp.dot(
        lax.all_gather(gradients, "seq", axis=0, tiled=True),
        projection,
        preferred_element_type=jnp.float32,
    )
    partial_value = partial_value.reshape(groups, layers, quarter, projection.shape[1])
    summed = lax.psum_scatter(partial_value, "layer", scatter_dimension=1, tiled=True)
    sketch = summed.reshape(groups * quarter, projection.shape[1]).astype(jnp.bfloat16)
    sketch_wide = sketch.astype(jnp.float32)
    row_squares = lax.psum_scatter(
        jnp.sum(sketch_wide * sketch_wide, axis=1), "seq", scatter_dimension=0, tiled=True
    )
    query_wide = queries.astype(jnp.float32)
    query_squares = lax.psum(jnp.sum(query_wide * query_wide, axis=1), "seq")
    products = lax.psum_scatter(
        lax.dot_general(
            sketch, queries, (((1,), (1,)), ((), ())), preferred_element_type=jnp.float32
        ),
        "seq",
        scatter_dimension=0,
        tiled=True,
    )
    width = projection.shape[1] * groups
    return scaled(width, products, row_squares[:, None], query_squares[None, :])


def shards(gradients, projection, queries):
    layers = lax.axis_size("layer")
    groups = lax.axis_size("seq")
    rows = gradients.shape[0] // layers
    needed = sum(
        math.prod(shape) * jnp.dtype(kind).itemsize
        for shape, kind in scratch(
            groups, layers, gradients.shape, projection.shape, queries.shape
        )
    )
    fits = (
        groups % 2 == 0
        and layers % 2 == 0
        and rows % 16 == 0
        and rows <= min(128, queries.shape[0])
        and needed < VMEM_BYTES - 8 * 2**20
    )
    path = fused if fits else plain
    return path(groups, layers, gradients, projection, queries)


def solution(mesh):
    placed = (P("seq", "layer"), P("layer", "seq"), P(None, "seq"))
    return jax.shard_map(
        shards, mesh=mesh, in_specs=placed, out_specs=P(("seq", "layer"), None), check_vma=False
    )
```

```python
import functools
import math

import jax
import jax.numpy as jnp
from jax import lax
from jax.experimental import pallas as pl
from jax.experimental.pallas import tpu as pltpu
from jax.sharding import PartitionSpec as P

epsilon = 1e-06
VMEM_BYTES = 60 * 2**20
MESH = pl.DeviceIdType.MESH


def scaled(width, products, row_squares, query_squares):
    return (
        math.sqrt(width)
        * products
        * lax.rsqrt(row_squares + epsilon)
        * lax.rsqrt(query_squares + epsilon)
    )


def kernel(
    groups, layers,
    g_hbm, p_hbm, q_hbm, out_ref,
    p_ref, q_ref, gbuf, pother, qt, totals, xsend, xrecv, sbuf, rbuf, mine,
    local_sem, core_sem, pair_sem, gsend, grecv, xsend_sem, xrecv_sem, rsend_sem, rrecv_sem,
):
    inner = 2
    outer = groups // inner
    banks = layers // 2
    rows = g_hbm.shape[2]
    columns = p_ref.shape[1]
    asked = q_ref.shape[0]
    me, layer = lax.axis_index("seq"), lax.axis_index("layer")
    z, y = me // inner, me % inner
    x, c = layer // 2, layer % 2
    partner = x * 2 + 1 - c

    own = pltpu.make_async_copy(g_hbm.at[:, c], gbuf.at[me, 0], local_sem.at[0])
    own.start()
    load_p = pltpu.make_async_copy(p_hbm, p_ref, local_sem.at[1])
    load_p.start()
    load_q = pltpu.make_async_copy(q_hbm, q_ref, local_sem.at[2])
    load_q.start()

    barrier = pltpu.get_barrier_semaphore()

    def greet(group, layer_to):
        pl.semaphore_signal(
            barrier, inc=1, device_id=(group, layer_to), device_id_type=MESH
        )

    greet(me, partner)
    greet(z * inner + 1 - y, layer)
    for step in range(1, banks):
        greet(me, (x + step) % banks * 2 + c)

    @pl.when(z > 0)
    def _():
        greet(me - inner, layer)

    @pl.when(z < outer - 1)
    def _():
        greet(me + inner, layer)

    ends = jnp.minimum(z, 1) + jnp.minimum(outer - 1 - z, 1)
    pl.semaphore_wait(barrier, banks + 1 + ends)

    def remote(src, dst, send, recv, group, layer_to):
        return pltpu.make_async_remote_copy(
            src_ref=src, dst_ref=dst, send_sem=send, recv_sem=recv,
            device_id=(group, layer_to), device_id_type=MESH,
        )

    swap_g = remote(
        g_hbm.at[:, 1 - c], gbuf.at[me, 1], core_sem, grecv.at[me, 1], me, partner
    )
    swap_g.start()

    reach = jnp.minimum(z, outer - 1 - z)

    def source(t):
        half = (t + 1) // 2
        side = jnp.where(2 * z < outer, 1, -1)
        near = z + side * half * (2 * (t % 2) - 1)
        far = jnp.where(z <= outer - 1 - z, t, outer - 1 - t)
        return jnp.where(t <= 2 * reach, near, far)

    def chunk(block, part, link, group):
        return remote(
            gbuf.at[block, part], gbuf.at[block, part],
            gsend.at[block, part, link], grecv.at[block, part], group, layer,
        )

    up, down = z < outer - 1, z > 0

    def relay(src, part, act):
        block = src * inner + y

        @pl.when((part == 0) | (src == z) | ((src > 0) & (src < outer - 1)))
        def _():
            act(chunk(block, part, 0, z * inner + 1 - y))

        @pl.when((src <= z) & up)
        def _():
            act(chunk(block, part, 1, me + inner))

        @pl.when((src >= z) & down)
        def _():
            act(chunk(block, part, 2, me - inner))

    def relay_other(src, act):
        block = src * inner + 1 - y

        @pl.when((src == 0) & up)
        def _():
            act(chunk(block, 1, 1, me + inner))

        @pl.when((src == outer - 1) & down)
        def _():
            act(chunk(block, 1, 2, me - inner))

    def start(copy):
        copy.start()

    def drain(copy):
        copy.wait_send()

    tile = min(columns, 256)

    def multiply(block):
        @pl.loop(0, columns // tile)
        def _(k):
            cols = pl.ds(pl.multiple_of(k * tile, tile), tile)
            first = gbuf[block, 0].reshape(banks * rows, -1)
            second = gbuf[block, 1].reshape(banks * rows, -1)
            total = jnp.dot(first, p_ref[:, cols], preferred_element_type=jnp.float32)
            total += jnp.dot(second, pother[:, cols], preferred_element_type=jnp.float32)
            total = total.reshape(banks, rows, tile)
            totals[block, :, :, cols] = total
            xsend[block, :, :, cols] = total.astype(jnp.bfloat16)

        for step in range(1, banks):
            exchange(block, step).start()

    def exchange(block, step):
        to = (x + step) % banks
        return remote(
            xsend.at[block, to], xrecv.at[block, step - 1],
            xsend_sem.at[block, step - 1], xrecv_sem.at[block, step - 1],
            me, to * 2 + c,
        )

    def deliver(block):
        return remote(
            sbuf.at[block], rbuf.at[me], rsend_sem.at[block], rrecv_sem.at[me], block, layer
        )

    def finish(block):
        sketch = totals[block, x]
        for step in range(1, banks):
            exchange(block, step).wait_recv()
            sketch += xrecv[block, step - 1].astype(jnp.float32)
        high = sketch.astype(jnp.bfloat16)
        low = (sketch - high.astype(jnp.float32)).astype(jnp.bfloat16)
        both = jnp.dot(
            jnp.concatenate([high, low], axis=0), qt[...], preferred_element_type=jnp.float32
        )
        squares = jnp.sum(sketch * sketch, axis=1, keepdims=True)
        products = both[:rows] + both[rows:]
        squares = jnp.broadcast_to(squares, (rows, 128)).T[:1]

        @pl.when(block == me)
        def _():
            mine[:rows] = products
            mine[rows : rows + 1, :rows] = squares

        @pl.when(block != me)
        def _():
            sbuf[block, :rows] = products.astype(jnp.bfloat16)
            pieces = jnp.concatenate(split(squares), axis=0)
            sbuf[block, rows : rows + 8, :rows] = pieces
            deliver(block).start()

    def split(exact):
        pieces = []
        for _ in range(3):
            piece = exact.astype(jnp.bfloat16)
            pieces.append(piece)
            exact -= piece.astype(jnp.float32)
        return pieces + [jnp.zeros((5, exact.shape[1]), jnp.bfloat16)]

    own.wait()
    relay(z, 0, start)
    swap_p = remote(p_hbm, pother, pair_sem.at[0], pair_sem.at[1], me, partner)
    swap_p.start()
    chunk(me, 1, 0, me).wait_recv()
    relay(z, 1, start)
    load_q.wait()

    wide = q_ref[...].T
    qt[...] = wide
    wide = wide.astype(jnp.float32)
    query_part = jnp.sum(wide * wide, axis=0, keepdims=True)

    mine[rows:] = jnp.zeros((16, asked), jnp.float32)
    mine[rows + 8 : rows + 9] = query_part
    query_pieces = jnp.concatenate(split(query_part), axis=0)

    @pl.loop(0, groups)
    def _(block):
        sbuf[block, rows + 8 :] = query_pieces

    load_p.wait()
    swap_p.wait_recv()

    lag = 1 + jnp.minimum(reach, 1)

    @pl.loop(0, outer + 3)
    def _(t):
        @pl.when(t < outer)
        def _():
            src = source(t)
            block = src * inner + y
            @pl.when(t > 0)
            def _():
                for part in range(2):
                    chunk(block, part, 0, me).wait_recv()
                    relay(src, part, start)

            multiply(block)

        @pl.when((t >= 1) & (t <= outer))
        def _():
            finish(source(t - 1) * inner + y)

        @pl.when((t >= lag) & (t < lag + outer))
        def _():
            src = source(t - lag)
            block = src * inner + 1 - y
            for part in range(2):
                chunk(block, part, 0, me).wait_recv()
            relay_other(src, start)
            multiply(block)

        @pl.when((t > lag) & (t <= lag + outer))
        def _():
            finish(source(t - lag - 1) * inner + 1 - y)

    products = mine[...]

    def collect(step, total):
        block = (me + step) % groups
        remote(
            sbuf.at[block], rbuf.at[block], rsend_sem.at[block], rrecv_sem.at[block],
            block, layer,
        ).wait_recv()
        return total + rbuf[block].astype(jnp.float32)

    products = lax.fori_loop(1, groups, collect, products)
    squares = products[rows : rows + 8, :rows].sum(axis=0, keepdims=True)
    squares = jnp.broadcast_to(squares, (128, rows)).T[:, :1]
    out_ref[...] = scaled(
        columns * groups, products[:rows], squares, products[rows + 8 :].sum(axis=0, keepdims=True)
    )

    swap_g.wait_send()
    swap_p.wait_send()

    @pl.loop(0, outer)
    def _(t):
        src = source(t)
        for part in range(2):
            relay(src, part, drain)
        relay_other(src, drain)

    @pl.loop(0, groups)
    def _(block):
        for step in range(1, banks):
            exchange(block, step).wait_send()

        @pl.when(block != me)
        def _():
            deliver(block).wait_send()


def scratch(groups, layers, gradients, projection, queries):
    banks, rows = layers // 2, gradients[0] // layers
    features, columns = projection
    asked = queries[0]
    message = (groups, rows + 16, asked)
    return [
        ((features, columns), jnp.bfloat16),
        ((asked, columns), jnp.bfloat16),
        ((groups, 2, banks, rows, features), jnp.bfloat16),
        ((features, columns), jnp.bfloat16),
        ((columns, asked), jnp.bfloat16),
        ((groups, banks, rows, columns), jnp.float32),
        ((groups, banks, rows, columns), jnp.bfloat16),
        ((groups, max(banks - 1, 1), rows, columns), jnp.bfloat16),
        (message, jnp.bfloat16),
        (message, jnp.bfloat16),
        (message[1:], jnp.float32),
    ]


def fused(groups, layers, gradients, projection, queries):
    banks = layers // 2
    rows = gradients.shape[0] // layers
    buffers = scratch(groups, layers, gradients.shape, projection.shape, queries.shape)
    dma = pltpu.SemaphoreType.DMA
    spread = max(banks - 1, 1)
    return pl.pallas_call(
        functools.partial(kernel, groups, layers),
        out_shape=jax.ShapeDtypeStruct((rows, queries.shape[0]), jnp.float32),
        in_specs=[pl.BlockSpec(memory_space=pl.ANY)] * 3,
        out_specs=pl.BlockSpec(memory_space=pltpu.VMEM),
        scratch_shapes=[pltpu.VMEM(shape, kind) for shape, kind in buffers]
        + [
            dma((3,)), dma, dma((2,)), dma((groups, 2, 3)), dma((groups, 2)),
            dma((groups, spread)), dma((groups, spread)), dma((groups,)), dma((groups,)),
        ],
        compiler_params=pltpu.CompilerParams(
            collective_id=0, has_side_effects=True, vmem_limit_bytes=VMEM_BYTES
        ),
    )(gradients.reshape(banks, 2, rows, gradients.shape[1]), projection, queries)


def plain(groups, layers, gradients, projection, queries):
    quarter = gradients.shape[0] // layers
    partial_value = jnp.dot(
        lax.all_gather(gradients, "seq", axis=0, tiled=True),
        projection,
        preferred_element_type=jnp.float32,
    )
    partial_value = partial_value.reshape(groups, layers, quarter, projection.shape[1])
    summed = lax.psum_scatter(partial_value, "layer", scatter_dimension=1, tiled=True)
    sketch = summed.reshape(groups * quarter, projection.shape[1]).astype(jnp.bfloat16)
    sketch_wide = sketch.astype(jnp.float32)
    row_squares = lax.psum_scatter(
        jnp.sum(sketch_wide * sketch_wide, axis=1), "seq", scatter_dimension=0, tiled=True
    )
    query_wide = queries.astype(jnp.float32)
    query_squares = lax.psum(jnp.sum(query_wide * query_wide, axis=1), "seq")
    products = lax.psum_scatter(
        lax.dot_general(
            sketch, queries, (((1,), (1,)), ((), ())), preferred_element_type=jnp.float32
        ),
        "seq",
        scatter_dimension=0,
        tiled=True,
    )
    width = projection.shape[1] * groups
    return scaled(width, products, row_squares[:, None], query_squares[None, :])


def shards(gradients, projection, queries):
    layers = lax.axis_size("layer")
    groups = lax.axis_size("seq")
    rows = gradients.shape[0] // layers
    needed = sum(
        math.prod(shape) * jnp.dtype(kind).itemsize
        for shape, kind in scratch(
            groups, layers, gradients.shape, projection.shape, queries.shape
        )
    )
    fits = (
        groups % 2 == 0
        and layers % 2 == 0
        and rows % 16 == 0
        and rows <= min(128, queries.shape[0])
        and needed < VMEM_BYTES - 8 * 2**20
    )
    path = fused if fits else plain
    return path(groups, layers, gradients, projection, queries)


def solution(mesh):
    placed = (P("seq", "layer"), P("layer", "seq"), P(None, "seq"))
    return jax.shard_map(
        shards, mesh=mesh, in_specs=placed, out_specs=P(("seq", "layer"), None), check_vma=False
    )
```

```python
import functools
import math

import jax
import jax.numpy as jnp
from jax import lax
from jax.experimental import pallas as pl
from jax.experimental.pallas import tpu as pltpu
from jax.sharding import PartitionSpec as P

epsilon = 1e-06
VMEM_BYTES = 60 * 2**20
TILE = 512
MESH = pl.DeviceIdType.MESH


def scaled(width, products, row_squares, query_squares):
    return (
        math.sqrt(width)
        * products
        * lax.rsqrt(row_squares + epsilon)
        * lax.rsqrt(query_squares + epsilon)
    )


def kernel(
    groups, layers,
    g_hbm, p_hbm, q_hbm, out_ref,
    p_ref, q_ref, gbuf, pother, qt, totals, xsend, xrecv, sbuf, rbuf, mine,
    local_sem, core_sem, pair_sem, gsend, grecv, xsend_sem, xrecv_sem, rsend_sem, rrecv_sem,
):
    inner = 2
    outer = groups // inner
    banks = layers // 2
    rows = g_hbm.shape[2]
    columns = p_ref.shape[1]
    asked = q_ref.shape[0]
    me, layer = lax.axis_index("seq"), lax.axis_index("layer")
    z, y = me // inner, me % inner
    x, c = layer // 2, layer % 2
    partner = x * 2 + 1 - c

    own = pltpu.make_async_copy(g_hbm.at[:, c], gbuf.at[me, 0], local_sem.at[0])
    own.start()
    load_p = pltpu.make_async_copy(p_hbm, p_ref, local_sem.at[1])
    load_p.start()
    load_q = pltpu.make_async_copy(q_hbm, q_ref, local_sem.at[2])
    load_q.start()

    barrier = pltpu.get_barrier_semaphore()

    def greet(group, layer_to):
        pl.semaphore_signal(
            barrier, inc=1, device_id=(group, layer_to), device_id_type=MESH
        )

    greet(me, partner)
    greet(z * inner + 1 - y, layer)
    for step in range(1, banks):
        greet(me, (x + step) % banks * 2 + c)

    @pl.when(z > 0)
    def _():
        greet(me - inner, layer)

    @pl.when(z < outer - 1)
    def _():
        greet(me + inner, layer)

    ends = jnp.minimum(z, 1) + jnp.minimum(outer - 1 - z, 1)
    pl.semaphore_wait(barrier, banks + 1 + ends)

    def remote(src, dst, send, recv, group, layer_to):
        return pltpu.make_async_remote_copy(
            src_ref=src, dst_ref=dst, send_sem=send, recv_sem=recv,
            device_id=(group, layer_to), device_id_type=MESH,
        )

    swap_g = remote(
        g_hbm.at[:, 1 - c], gbuf.at[me, 1], core_sem, grecv.at[me, 1], me, partner
    )
    swap_g.start()

    reach = jnp.minimum(z, outer - 1 - z)

    def source(t):
        half = (t + 1) // 2
        side = jnp.where(2 * z < outer, 1, -1)
        near = z + side * half * (2 * (t % 2) - 1)
        far = jnp.where(z <= outer - 1 - z, t, outer - 1 - t)
        return jnp.where(t <= 2 * reach, near, far)

    def chunk(block, part, link, group):
        return remote(
            gbuf.at[block, part], gbuf.at[block, part],
            gsend.at[block, part, link], grecv.at[block, part], group, layer,
        )

    up, down = z < outer - 1, z > 0

    def relay(src, part, act):
        block = src * inner + y

        @pl.when((part == 0) | (src == z) | ((src > 0) & (src < outer - 1)))
        def _():
            act(chunk(block, part, 0, z * inner + 1 - y))

        @pl.when((src <= z) & up)
        def _():
            act(chunk(block, part, 1, me + inner))

        @pl.when((src >= z) & down)
        def _():
            act(chunk(block, part, 2, me - inner))

    def relay_other(src, act):
        block = src * inner + 1 - y

        @pl.when((src == 0) & up)
        def _():
            act(chunk(block, 1, 1, me + inner))

        @pl.when((src == outer - 1) & down)
        def _():
            act(chunk(block, 1, 2, me - inner))

    def start(copy):
        copy.start()

    def drain(copy):
        copy.wait_send()

    tile = min(columns, TILE)

    def part_product(block, part, weights, cols):
        left = gbuf[block, part].reshape(banks * rows, -1)
        product = jnp.dot(left, weights[:, cols], preferred_element_type=jnp.float32)
        return product.reshape(banks, rows, tile)

    def columns_of(k):
        return pl.ds(pl.multiple_of(k * tile, tile), tile)

    def begin(block):
        @pl.loop(0, columns // tile)
        def _(k):
            cols = columns_of(k)
            totals[block, :, :, cols] = part_product(block, 0, p_ref, cols)

    def complete(block):
        @pl.loop(0, columns // tile)
        def _(k):
            cols = columns_of(k)
            total = totals[block, :, :, cols] + part_product(block, 1, pother, cols)
            totals[block, :, :, cols] = total
            xsend[block, :, :, cols] = total.astype(jnp.bfloat16)
            for step in range(1, banks):
                exchange(block, step, k).start()

    def exchange(block, step, k):
        to = (x + step) % banks
        cols = columns_of(k)
        return remote(
            xsend.at[block, to, :, cols], xrecv.at[block, step - 1, :, cols],
            xsend_sem.at[block, step - 1, k], xrecv_sem.at[block, step - 1, k],
            me, to * 2 + c,
        )

    def deliver(block):
        return remote(
            sbuf.at[block], rbuf.at[me], rsend_sem.at[block], rrecv_sem.at[me], block, layer
        )

    def finish(block):
        sketch = totals[block, x]
        for step in range(1, banks):
            for k in range(columns // tile):
                exchange(block, step, k).wait_recv()
            sketch += xrecv[block, step - 1].astype(jnp.float32)
        high = sketch.astype(jnp.bfloat16)
        low = (sketch - high.astype(jnp.float32)).astype(jnp.bfloat16)
        both = jnp.dot(
            jnp.concatenate([high, low], axis=0), qt[...], preferred_element_type=jnp.float32
        )
        squares = jnp.sum(sketch * sketch, axis=1, keepdims=True)
        products = both[:rows] + both[rows:]
        squares = jnp.broadcast_to(squares, (rows, 128)).T[:1]

        @pl.when(block == me)
        def _():
            mine[:rows] = products
            mine[rows : rows + 1, :rows] = squares

        @pl.when(block != me)
        def _():
            sbuf[block, :rows] = products.astype(jnp.bfloat16)
            pieces = jnp.concatenate(split(squares), axis=0)
            sbuf[block, rows : rows + 8, :rows] = pieces
            deliver(block).start()

    def split(exact):
        pieces = []
        for _ in range(3):
            piece = exact.astype(jnp.bfloat16)
            pieces.append(piece)
            exact -= piece.astype(jnp.float32)
        return pieces + [jnp.zeros((5, exact.shape[1]), jnp.bfloat16)]

    own.wait()
    relay(z, 0, start)
    swap_p = remote(p_hbm, pother, pair_sem.at[0], pair_sem.at[1], me, partner)
    swap_p.start()
    chunk(me, 1, 0, me).wait_recv()
    relay(z, 1, start)
    load_q.wait()

    wide = q_ref[...].T
    qt[...] = wide
    wide = wide.astype(jnp.float32)
    query_part = jnp.sum(wide * wide, axis=0, keepdims=True)

    mine[rows:] = jnp.zeros((16, asked), jnp.float32)
    mine[rows + 8 : rows + 9] = query_part
    query_pieces = jnp.concatenate(split(query_part), axis=0)

    @pl.loop(0, groups)
    def _(block):
        sbuf[block, rows + 8 :] = query_pieces

    load_p.wait()
    swap_p.wait_recv()

    lag = 1 + jnp.minimum(reach, 1)

    @pl.loop(0, outer + 3)
    def _(t):
        @pl.when(t < outer)
        def _():
            src = source(t)
            block = src * inner + y
            @pl.when(t > 0)
            def _():
                for part in range(2):
                    chunk(block, part, 0, me).wait_recv()
                    relay(src, part, start)

            begin(block)
            complete(block)

        @pl.when((t >= 1) & (t <= outer))
        def _():
            finish(source(t - 1) * inner + y)

        @pl.when((t >= lag) & (t < lag + outer))
        def _():
            src = source(t - lag)
            block = src * inner + 1 - y
            chunk(block, 0, 0, me).wait_recv()
            begin(block)
            chunk(block, 1, 0, me).wait_recv()
            relay_other(src, start)
            complete(block)

        @pl.when((t > lag) & (t <= lag + outer))
        def _():
            finish(source(t - lag - 1) * inner + 1 - y)

    products = mine[...]

    def collect(step, total):
        block = (me + step) % groups
        remote(
            sbuf.at[block], rbuf.at[block], rsend_sem.at[block], rrecv_sem.at[block],
            block, layer,
        ).wait_recv()
        return total + rbuf[block].astype(jnp.float32)

    products = lax.fori_loop(1, groups, collect, products)
    squares = products[rows : rows + 8, :rows].sum(axis=0, keepdims=True)
    squares = jnp.broadcast_to(squares, (128, rows)).T[:, :1]
    out_ref[...] = scaled(
        columns * groups, products[:rows], squares, products[rows + 8 :].sum(axis=0, keepdims=True)
    )

    swap_g.wait_send()
    swap_p.wait_send()

    @pl.loop(0, outer)
    def _(t):
        src = source(t)
        for part in range(2):
            relay(src, part, drain)
        relay_other(src, drain)

    @pl.loop(0, groups)
    def _(block):
        for step in range(1, banks):
            for k in range(columns // tile):
                exchange(block, step, k).wait_send()

        @pl.when(block != me)
        def _():
            deliver(block).wait_send()


def scratch(groups, layers, gradients, projection, queries):
    banks, rows = layers // 2, gradients[0] // layers
    features, columns = projection
    asked = queries[0]
    message = (groups, rows + 16, asked)
    return [
        ((features, columns), jnp.bfloat16),
        ((asked, columns), jnp.bfloat16),
        ((groups, 2, banks, rows, features), jnp.bfloat16),
        ((features, columns), jnp.bfloat16),
        ((columns, asked), jnp.bfloat16),
        ((groups, banks, rows, columns), jnp.float32),
        ((groups, banks, rows, columns), jnp.bfloat16),
        ((groups, max(banks - 1, 1), rows, columns), jnp.bfloat16),
        (message, jnp.bfloat16),
        (message, jnp.bfloat16),
        (message[1:], jnp.float32),
    ]


def fused(groups, layers, gradients, projection, queries):
    banks = layers // 2
    rows = gradients.shape[0] // layers
    buffers = scratch(groups, layers, gradients.shape, projection.shape, queries.shape)
    dma = pltpu.SemaphoreType.DMA
    spread = max(banks - 1, 1)
    columns = projection.shape[1]
    tiles = columns // min(columns, TILE)
    return pl.pallas_call(
        functools.partial(kernel, groups, layers),
        out_shape=jax.ShapeDtypeStruct((rows, queries.shape[0]), jnp.float32),
        in_specs=[pl.BlockSpec(memory_space=pl.ANY)] * 3,
        out_specs=pl.BlockSpec(memory_space=pltpu.VMEM),
        scratch_shapes=[pltpu.VMEM(shape, kind) for shape, kind in buffers]
        + [
            dma((3,)), dma, dma((2,)), dma((groups, 2, 3)), dma((groups, 2)),
            dma((groups, spread, tiles)), dma((groups, spread, tiles)), dma((groups,)), dma((groups,)),
        ],
        compiler_params=pltpu.CompilerParams(
            collective_id=0, has_side_effects=True, vmem_limit_bytes=VMEM_BYTES
        ),
    )(gradients.reshape(banks, 2, rows, gradients.shape[1]), projection, queries)


def plain(groups, layers, gradients, projection, queries):
    quarter = gradients.shape[0] // layers
    partial_value = jnp.dot(
        lax.all_gather(gradients, "seq", axis=0, tiled=True),
        projection,
        preferred_element_type=jnp.float32,
    )
    partial_value = partial_value.reshape(groups, layers, quarter, projection.shape[1])
    summed = lax.psum_scatter(partial_value, "layer", scatter_dimension=1, tiled=True)
    sketch = summed.reshape(groups * quarter, projection.shape[1]).astype(jnp.bfloat16)
    sketch_wide = sketch.astype(jnp.float32)
    row_squares = lax.psum_scatter(
        jnp.sum(sketch_wide * sketch_wide, axis=1), "seq", scatter_dimension=0, tiled=True
    )
    query_wide = queries.astype(jnp.float32)
    query_squares = lax.psum(jnp.sum(query_wide * query_wide, axis=1), "seq")
    products = lax.psum_scatter(
        lax.dot_general(
            sketch, queries, (((1,), (1,)), ((), ())), preferred_element_type=jnp.float32
        ),
        "seq",
        scatter_dimension=0,
        tiled=True,
    )
    width = projection.shape[1] * groups
    return scaled(width, products, row_squares[:, None], query_squares[None, :])


def shards(gradients, projection, queries):
    layers = lax.axis_size("layer")
    groups = lax.axis_size("seq")
    rows = gradients.shape[0] // layers
    needed = sum(
        math.prod(shape) * jnp.dtype(kind).itemsize
        for shape, kind in scratch(
            groups, layers, gradients.shape, projection.shape, queries.shape
        )
    )
    fits = (
        groups % 2 == 0
        and layers % 2 == 0
        and rows % 16 == 0
        and projection.shape[1] % min(projection.shape[1], TILE) == 0
        and min(projection.shape[1], TILE) % 128 == 0
        and rows <= min(128, queries.shape[0])
        and needed < VMEM_BYTES - 8 * 2**20
    )
    path = fused if fits else plain
    return path(groups, layers, gradients, projection, queries)


def solution(mesh):
    placed = (P("seq", "layer"), P("layer", "seq"), P(None, "seq"))
    return jax.shard_map(
        shards, mesh=mesh, in_specs=placed, out_specs=P(("seq", "layer"), None), check_vma=False
    )
```
